32 devices in a mesh: replica: 4 (over x, core), fsdp: 8 (over z, y).
Axes of the slice: x: 2, y: 2, z: 4, core: 2. Of those that a mesh axis runs over, the one named last changes fastest.
Arguments:
- anchor: float32 [1536, 1536], P('fsdp', 'replica'), may hold values from -0.15625 to 0.15625
- momentum: float32 [1536, 1536], P('fsdp', 'replica'), may hold values from -0.75 to 0.75
- change: float32 [4, 1536, 1536], P('replica', 'fsdp'), may hold values from -0.75 to 0.75
- adam_first: float32 [4, 1536, 1536], P('replica', 'fsdp'), may hold values from -4 to 4
- adam_second: float32 [4, 1536, 1536], P('replica', 'fsdp'), may hold values from 0.1 to 2
- attn_out: bfloat16 [4, 8192, 1536], P('replica', 'fsdp'), may hold values from -6 to 6
- grad_out: bfloat16 [4, 8192, 1536], P('replica', 'fsdp'), may hold values from -6 to 6
Outputs:
- new_anchor: float32 [1536, 1536], P('fsdp', 'replica')
- new_momentum: float32 [1536, 1536], P('fsdp', 'replica')
- new_local: float32 [4, 1536, 1536], P('replica', 'fsdp')
- new_first: float32 [4, 1536, 1536], P('replica', 'fsdp')
- new_second: float32 [4, 1536, 1536], P('replica', 'fsdp')
- input_grad: bfloat16 [4, 8192, 1536], P('replica', 'fsdp')
The draws below stay inside these ranges and needn't reach their ends.
All inputs are finite; a program needn't handle non-finite values.
Results may differ from the reference program's by a relative error of at most 0.0049.
Values may be sent and summed in bfloat16 or wider, within the bound.
A program may use at most 128 MiB of HBM per device.

```python
import math
import jax
import jax.numpy as jnp
from jax import lax

D = 1536
REPLICAS = 4
TOKENS = 8192


def spiked(values, key, source, target, shards_of, factor):
    owner, partner = [(jnp.arange(values.shape[dim]) // (values.shape[dim] // shards_of)).reshape([-1 if axis == dim else 1 for axis in range(values.ndim)]) for dim in (source, target)]
    chosen = jax.random.permutation(key, shards_of)[partner]
    strong = (owner == chosen) | (owner == (partner + shards_of // 2) % shards_of)
    return jnp.where(strong, factor * values, values)


def shard_levels(own_key, dims, split, smallest, top_value):
    gain, own = 1.0, jax.random.fold_in(own_key, 6)
    for position, shards_of in split:
        steps = jnp.exp(jax.random.uniform(jax.random.fold_in(own, position), (shards_of,), jnp.float32, smallest / len(split), top_value / len(split)))
        gain = gain * jnp.repeat(steps, dims[position] // shards_of).reshape([-1 if axis == position else 1 for axis in range(len(dims))])
    return gain


def gaussian(own_key, extent, spread, limit, split=(), dtype=jnp.bfloat16):
    result = jax.random.normal(own_key, extent, jnp.float32) * spread
    if len(split) > 0:
        result = shard_levels(own_key, extent, split, -0.22, 0.18) * result
    return jnp.clip(result, min=-limit, max=limit).astype(dtype)


def bell_draw_with(stream_key, extent, deviation, most, cuts, heavy, held_as=jnp.bfloat16):
    result = deviation * jax.random.normal(stream_key, extent, jnp.float32)
    if cuts:
        result = result * shard_levels(stream_key, extent, cuts, -0.22, 0.18)
    return jnp.clip(spiked(result, jax.random.fold_in(stream_key, 3), *heavy), -most, most).astype(held_as)


def setup_inputs(seed: int = 0) -> dict:
    seeds = jax.random.split(jax.random.key(seed), 8)
    return {
        "anchor": gaussian(seeds[0], (D, D), D ** -0.5, 0.15625, ((0, 8), (1, 4)), jnp.float32),
        "momentum": gaussian(seeds[1], (D, D), 0.05, 0.75, ((0, 8), (1, 4)), jnp.float32),
        "change": gaussian(seeds[2], (REPLICAS, D, D), 0.05, 0.75, ((0, 4), (1, 8)), jnp.float32),
        "adam_first": gaussian(seeds[3], (REPLICAS, D, D), 0.3, 4.0, ((0, 4), (1, 8)), jnp.float32),
        "adam_second": jnp.clip(jnp.exp(math.log(2.0) - 2.9957323 * jax.random.uniform(seeds[4], (REPLICAS, D, D), jnp.float32) ** shard_levels(seeds[4], (REPLICAS, D, D), ((0, 4), (1, 8)), -0.2, 0.2)), 0.1, 2.0),
        "attn_out": bell_draw_with(seeds[5], (REPLICAS, TOKENS, D), 1.0, 6.0, ((0, 4), (1, 8)), (1, 2, 8, 2.0)),
        "grad_out": gaussian(seeds[6], (REPLICAS, TOKENS, D), 1.0, 6.0, ((0, 4), (1, 8))),
    }


outer_rate = 0.7
outer_mu = 0.9
inner_rate = 0.005
beta_one = 0.9
beta_two = 0.95
decay_rate = 0.1
epsilon = 1e-08

def reference(anchor, momentum, change, adam_first, adam_second, attn_out, grad_out):
    outer_grad = -lax.optimization_barrier(jnp.sum(change, axis=0)) / REPLICAS
    new_momentum = outer_mu * momentum + outer_grad
    new_anchor = anchor - outer_rate * (outer_grad + outer_mu * new_momentum)
    weights = new_anchor.astype(jnp.bfloat16)
    grad_scale = TOKENS ** (-0.5)

    def one_group(operands):
        inputs, cotangent, first, second = operands
        gradient = jnp.dot(inputs.T, cotangent, preferred_element_type=jnp.float32) * grad_scale
        first_next = beta_one * first + (1.0 - beta_one) * gradient
        second_next = beta_two * second + (1.0 - beta_two) * gradient * gradient
        local = new_anchor - inner_rate * (first_next / (jnp.sqrt(second_next) + epsilon) + decay_rate * new_anchor)
        back = jnp.dot(cotangent, weights.T, preferred_element_type=jnp.float32).astype(jnp.bfloat16)
        return (local, first_next, second_next, back)
    results = lax.map(one_group, (attn_out, grad_out, adam_first, adam_second))
    return (new_anchor, new_momentum, results[0], results[1], results[2], results[3])
```

```python
import functools

import jax
import jax.numpy as jnp
from jax import lax
from jax.experimental import pallas as pl
from jax.experimental.pallas import tpu as pltpu
from jax.sharding import PartitionSpec as P

outer_rate = 0.7
outer_mu = 0.9
inner_rate = 0.005
beta_one = 0.9
beta_two = 0.95
decay_rate = 0.1
epsilon = 1e-08

MESH = pl.DeviceIdType.MESH
f32 = jnp.float32
bf16 = jnp.bfloat16


def adam(anchor_next, first, second, gradient):
    first_next = beta_one * first + (1.0 - beta_one) * gradient
    second_next = beta_two * second + (1.0 - beta_two) * gradient * gradient
    local = anchor_next - inner_rate * (
        first_next / (jnp.sqrt(second_next) + epsilon) + decay_rate * anchor_next
    )
    return local, first_next, second_next


def outer_step(anchor, momentum, summed, groups):
    outer_grad = -summed / groups
    new_momentum = outer_mu * momentum + outer_grad
    new_anchor = anchor - outer_rate * (outer_grad + outer_mu * new_momentum)
    return new_anchor, new_momentum


def plain_shards(anchor, momentum, change, adam_first, adam_second, attn_out, grad_out):
    groups = lax.axis_size("replica")
    summed = lax.psum_scatter(change[0], "replica", scatter_dimension=1, tiled=True)
    new_anchor, new_momentum = outer_step(anchor, momentum, summed, groups)
    anchor_next = lax.all_gather(new_anchor, "replica", axis=1, tiled=True)
    inputs, cotangent = attn_out[0], grad_out[0]
    grad_scale = (inputs.shape[0] * lax.axis_size("fsdp")) ** (-0.5)
    gradient = grad_scale * lax.psum_scatter(
        lax.dot_general(inputs, cotangent, (((0,), (0,)), ((), ())), preferred_element_type=f32),
        "fsdp",
        scatter_dimension=0,
        tiled=True,
    )
    input_grad = lax.dot_general(
        cotangent,
        lax.all_gather(anchor_next.astype(bf16), "fsdp", axis=0, tiled=True),
        (((1,), (1,)), ((), ())),
        preferred_element_type=f32,
    ).astype(bf16)
    local, first, second = adam(anchor_next, adam_first[0], adam_second[0], gradient)
    return new_anchor, new_momentum, local[None], first[None], second[None], input_grad[None]


INNER_STEPS = (
    "own", "L0", "ab0", "L1", "aa0", "y11", "y21", "ao1", "y31", "L2", "y10", "aa1", "ac0", "xo1", "S01",
    "xa0", "ab1", "ac1", "S00", "xa1", "y30", "S21", "xb0", "S11", "xc0", "CL", "S20", "xb1", "xc1", "S10",
    "Ma", "Mb", "Mc", "xo0", "FL", "Mo", "F1", "F0",
)
OUTER_STEPS = (
    "own", "S01", "ab0", "xo0", "ac0", "S00", "C0", "S11", "ab1", "S10", "L2", "xb0", "ao1", "ad0", "S21",
    "ac1", "ad1", "xc0", "xo1", "xd0", "xc1", "xb1", "CL", "S20", "Mo", "xd1", "Mc", "Mb", "Md", "FL", "F1",
    "F0",
)
ROUTES = {
    True: {"o0": "bayxs", "a0": "ybxs", "o1": "abxs", "a1": "abxs"},
    False: {"o0": "bxs"},
}
LONE = {True: "axs", False: "xs"}


def kernel(
    depth, groups, scale, lead, cuts,
    anchor_hbm, momentum_hbm, change_hbm, attn_hbm, cot_hbm,
    summed_ref, row_ref, grad_ref, back,
    anchor, momentum, change, attn, cot, flipped,
    part, got, own, other, psend, ry, zsend, chain, weights,
    lead_own, lead_send, lead_chain, lead_out, lead_in,
    local_sem, part_s, part_r, py_s, py_r, ch_s, ch_r,
    lz_s, lz_r, ly_s, ly_r, ag_s, ag_r,
):
    r = lax.axis_index("replica")
    f = lax.axis_index("fsdp")
    x, core = r // 2, r % 2
    z, y = f // 2, f % 2
    over_x, over_y = 1 - x, 1 - y
    rows, width = change.shape
    cols = width // groups
    pair = 2 * rows
    last = depth - 1
    pieces = len(cuts)
    inner = jnp.logical_and(z > 0, z < last)
    low = z < depth // 2
    inward = z + jnp.where(low, 1, -1)
    outward = z - jnp.where(low, 1, -1)
    places = {
        True: {"o": z, "a": outward, "b": inward, "c": last - outward},
        False: {"o": z, "b": inward, "c": last - inward, "d": last - z},
    }
    flip_y = {"replica": r, "fsdp": z * 2 + over_y}
    sibling = {"replica": x * 2 + (1 - core), "fsdp": f}
    to_inward = {"replica": r, "fsdp": inward * 2 + y}
    to_outward = {"replica": r, "fsdp": outward * 2 + y}
    links = {
        "a": to_outward, "b": to_inward, "y": flip_y, "s": sibling,
        "x": {"replica": over_x * 2 + core, "fsdp": f},
    }

    loads = []
    for i, (src, dst) in enumerate((
        (change_hbm, change), (attn_hbm, attn), (cot_hbm, cot),
        (anchor_hbm, anchor), (momentum_hbm, momentum),
    )):
        loads.append(pltpu.make_async_copy(src, dst, local_sem.at[i]))
        loads[-1].start()

    barrier = pltpu.get_barrier_semaphore()
    for k in range(1, groups):
        pl.semaphore_signal(
            barrier, inc=1, device_id={"replica": (r + k) % groups, "fsdp": f}, device_id_type=MESH
        )
    pl.semaphore_signal(barrier, inc=1, device_id=flip_y, device_id_type=MESH)
    pl.semaphore_signal(barrier, inc=1, device_id=to_inward, device_id_type=MESH)

    @pl.when(inner)
    def _():
        pl.semaphore_signal(barrier, inc=1, device_id=to_outward, device_id_type=MESH)

    def remote(src, dst, send, recv, device):
        return pltpu.make_async_remote_copy(
            src_ref=src, dst_ref=dst, send_sem=send, recv_sem=recv,
            device_id=device, device_id_type=MESH,
        )

    loads[0].wait()
    for k in range(1, groups):
        at = pl.multiple_of(((r + k) % groups) * cols, 128)
        part[k] = change[:, pl.ds(at, cols)].astype(bf16)
    pl.semaphore_wait(barrier, groups + 1 + jnp.where(inner, 1, 0))
    parts = []
    for k in range(1, groups):
        parts.append(remote(
            part.at[k], got.at[k - 1], part_s.at[k - 1], part_r.at[k - 1],
            {"replica": (r + k) % groups, "fsdp": f},
        ))
        parts[-1].start()

    def block_at(i):
        lower = jnp.where(i < last - z, last - i, i - (last - z))
        upper = jnp.where(i < z, i, last - (i - z))
        return jnp.where(low, lower, upper)

    lines = 16

    def by_rows(body, count):
        def step(j, carry):
            body(pl.ds(pl.multiple_of(j * lines, lines), lines))
            return carry

        lax.fori_loop(0, count // lines, step, 0)

    def piece(h):
        return pl.ds(*cuts[h])

    def y_copy(i, h):
        return remote(
            psend.at[i, :, piece(h)], ry.at[i, :, piece(h)],
            py_s.at[pieces * i + h], py_r.at[pieces * i + h], flip_y,
        )

    def route(inside, i):
        if not inside:
            return i, to_inward
        return (depth - 1 + i, to_inward) if i < 2 else (depth - 1, to_outward)

    def lead_copy(inside, i):
        slot, device = route(inside, i)
        return remote(lead_send.at[i], lead_chain.at[slot], lz_s.at[i], lz_r.at[slot], device)

    def z_copy(inside, i, h):
        slot, device = route(inside, i)
        return remote(
            zsend.at[i, :, piece(h)], chain.at[slot, :, piece(h)],
            ch_s.at[pieces * i + h], ch_r.at[pieces * slot + h], device,
        )

    def extra_copy(h):
        return remote(
            psend.at[2, :, piece(h)], chain.at[depth, :, piece(h)],
            ch_s.at[pieces * last + h], ch_r.at[pieces * depth + h], to_outward,
        )

    def lead_arrived(slot):
        remote(
            lead_send.at[0], lead_chain.at[slot], lz_s.at[0], lz_r.at[slot], flip_y
        ).wait_recv()

    def z_arrived(slot, h):
        remote(
            zsend.at[0, :, piece(h)], chain.at[slot, :, piece(h)],
            ch_s.at[h], ch_r.at[pieces * slot + h], flip_y,
        ).wait_recv()

    sends = {True: [], False: []}

    def start(inside, make):
        make().start()
        sends[inside].append(make)

    loads[1].wait()
    loads[2].wait()

    def multiply(i, carry):
        at = pl.multiple_of(block_at(i) * pair, 128)
        flipped[...] = attn[:, pl.ds(at, pair)].T
        for h in range(pieces):
            product = jnp.dot(flipped[...], cot[:, piece(h)], preferred_element_type=f32)
            upper, lower = product[:rows], product[rows:]
            own[i, :, piece(h)] = jnp.where(y == 0, upper, lower)
            across = jnp.where(y == 0, lower, upper)
            psend[i, :, piece(h)] = across.astype(bf16)

            @pl.when(i == last)
            def _():
                other[:, piece(h)] = across

            early = jnp.where(inner, i == 0, i < last if h == 0 else i <= last)

            @pl.when(early)
            def _():
                y_copy(i, h).start()

            if h == 0:
                @pl.when(jnp.logical_and(inner, i == 2))
                def _():
                    extra_copy(h).start()

        lead_own[i] = jnp.dot(flipped[...], cot[:, :lead], preferred_element_type=f32)

        @pl.when(jnp.logical_and(jnp.logical_not(inner), i < last))
        def _():
            lead_send[i] = lead_own[i].astype(bf16)

            @pl.when(i < 2)
            def _():
                lead_copy(False, i).start()

        return carry

    lax.fori_loop(0, depth, multiply, 0)
    for h in range(pieces):
        sends[True].append(functools.partial(y_copy, 0, h))
        for i in range(depth if h else last):
            sends[False].append(functools.partial(y_copy, i, h))
    sends[True].append(functools.partial(extra_copy, 0))
    for i in range(2):
        sends[False].append(functools.partial(lead_copy, False, i))

    loads[3].wait()
    loads[4].wait()
    for k in range(1, groups):
        parts[k - 1].wait_recv()
    mine = pl.ds(pl.multiple_of(r * cols, 128), cols)
    total = change[:, mine]
    for k in range(1, groups):
        total = total + got[k - 1].astype(f32)
    summed_ref[...] = total
    weights[f, :, mine] = outer_step(anchor[...], momentum[...], total, groups)[0].astype(bf16)

    def shard_copy(where, index, device):
        zs, ys, xs, cs = where
        at = pl.multiple_of((xs * 2 + cs) * cols, 128)
        ref = weights.at[zs * 2 + ys, :, pl.ds(at, cols)]
        return remote(
            ref, ref, ag_s.at[index], ag_r.at[((zs * 2 + ys) * 2 + xs) * 2 + cs], device
        )

    def arrived(where):
        shard_copy(where, 0, sibling).wait_recv()

    used = {True: 0, False: 0}

    def spread(inside, where, names):
        for name in names:
            start(inside, functools.partial(shard_copy, where, used[inside], links[name]))
            used[inside] += 1

    def lead_step(inside, i):
        if inside:
            slot = i if i < 2 else depth - 1
            lead_arrived(slot)

            def add(there):
                lead_send[i, there] = (
                    lead_own[i, there] + lead_chain[slot, there].astype(f32)
                ).astype(bf16)

            by_rows(add, pair)
        start(inside, functools.partial(lead_copy, inside, i))

    def chain_step(inside, i, h):
        crossed = not inside or i < 2 or h > 0
        slot = i if i < 2 else depth - 1
        if crossed:
            y_copy(i, h).wait_recv()
        if inside:
            z_arrived(slot, h)

        def add(there):
            value = own[i, there, piece(h)]
            if crossed:
                value = value + ry[i, there, piece(h)].astype(f32)
            if inside:
                value = value + chain[slot, there, piece(h)].astype(f32)
            zsend[i, there, piece(h)] = value.astype(bf16)

        by_rows(add, rows)
        start(inside, functools.partial(z_copy, inside, i, h))

    def cross_step(h):
        z_arrived(depth, h)

        def add(there):
            psend[last, there, piece(h)] = (
                other[there, piece(h)] + chain[depth, there, piece(h)].astype(f32)
            ).astype(bf16)

        by_rows(add, rows)
        start(False, functools.partial(y_copy, last, h))

    ends = {True: (2, depth), False: (depth - 1,)}

    def lead_swap():
        return remote(lead_out, lead_in, ly_s.at[0], ly_r.at[0], flip_y)

    away = pl.multiple_of((1 - y) * rows, 8)
    home = pl.multiple_of(y * rows, 8)

    def cross_lead(inside):
        for slot in ends[inside]:
            lead_arrived(slot)
        value = lead_own[last, pl.ds(away, rows)]
        for slot in ends[inside]:
            value = value + lead_chain[slot, pl.ds(away, rows)].astype(f32)
        lead_out[...] = value.astype(bf16)
        start(inside, lead_swap)

    def finish_lead(inside):
        lead_swap().wait_recv()
        value = lead_own[last, pl.ds(home, rows)] + lead_in[...].astype(f32)
        for slot in ends[inside]:
            value = value + lead_chain[slot, pl.ds(home, rows)].astype(f32)
        grad_ref[:, :lead] = value * scale

    def finish(inside, h):
        y_copy(last, h).wait_recv()
        for slot in ends[inside]:
            z_arrived(slot, h)

        def add(there):
            value = own[last, there, piece(h)] + ry[last, there, piece(h)].astype(f32)
            for slot in ends[inside]:
                value = value + chain[slot, there, piece(h)].astype(f32)
            grad_ref[there, piece(h)] = value * scale

        by_rows(add, rows)

    def take(inside, step):
        kind, spot = step[0], step[1:]
        if step == "own":
            spread(inside, (z, y, x, core), ROUTES[inside]["o0"])
        elif kind in "ax":
            zs, ys = places[inside][spot[0]], y if spot[1] == "0" else over_y
            if kind == "a":
                where = (zs, ys, x, core)
                arrived(where)
                spread(inside, where, ROUTES[inside].get(spot, LONE[inside]))
            else:
                where = (zs, ys, over_x, core)
                arrived(where)
                spread(inside, where, "s")
        elif kind == "L":
            lead_step(inside, int(spot))
        elif kind == "S":
            chain_step(inside, int(spot[0]), int(spot[1]))
        elif kind == "y":
            start(inside, functools.partial(y_copy, int(spot[0]), int(spot[1])))
        elif step == "CL":
            cross_lead(inside)
        elif kind == "C":
            cross_step(int(spot))
        elif step == "FL":
            finish_lead(inside)
        elif kind == "F":
            finish(inside, int(spot))

    runs, outs = {}, {}
    for inside, steps in ((True, INNER_STEPS), (False, OUTER_STEPS)):
        runs[inside], outs[inside] = [[]], []
        for step in steps:
            if step[0] == "M":
                outs[inside].append(places[inside][step[1]])
                runs[inside].append([])
            else:
                runs[inside][-1].append(step)

    for k in range(depth + 1):
        for inside in (True, False):
            @pl.when(inner if inside else jnp.logical_not(inner))
            def _():
                for step in runs[inside][k]:
                    take(inside, step)

        if k < depth:
            zs = jnp.where(inner, outs[True][k], outs[False][k])
            for ys in range(2):
                for xs in range(2):
                    arrived((zs, ys, xs, 1 - core))
            there = pl.ds(pl.multiple_of(zs * pair, 128), pair)
            block = weights[pl.ds(2 * zs, 2)].reshape(pair, width)
            back[:, there] = lax.dot_general(
                cot[...], block, (((1,), (1,)), ((), ())), preferred_element_type=f32
            ).astype(bf16)

    row_ref[...] = weights[f]
    for copy in parts:
        copy.wait_send()
    for inside in (True, False):
        @pl.when(inner if inside else jnp.logical_not(inner))
        def _():
            for make in sends[inside]:
                make().wait_send()


def finish_kernel(
    groups, lines,
    anchor, momentum, summed, row, first, second, gradient, back,
    anchor_hbm, momentum_hbm, local_hbm, first_hbm, second_hbm, back_hbm,
    anchor_out, momentum_out, local_out, first_out, second_out, sems,
):
    copies = []

    def put(src, dst):
        copies.append(pltpu.make_async_copy(src, dst, sems.at[len(copies)]))
        copies[-1].start()

    put(back, back_hbm)
    for k in range(row.shape[0] // lines):
        there = pl.ds(k * lines, lines)
        local, first_next, second_next = adam(
            row[there].astype(f32), first[there], second[there], gradient[there]
        )
        first_out[there] = first_next
        put(first_out.at[there], first_hbm.at[there])
        second_out[there] = second_next
        put(second_out.at[there], second_hbm.at[there])
        local_out[there] = local
        put(local_out.at[there], local_hbm.at[there])
    new_anchor, new_momentum = outer_step(anchor[...], momentum[...], summed[...], groups)
    anchor_out[...] = new_anchor
    put(anchor_out, anchor_hbm)
    momentum_out[...] = new_momentum
    put(momentum_out, momentum_hbm)
    for copy in copies:
        copy.wait()


def plan(width):
    lead = width // 6 // 128 * 128
    half = (width - lead) // 256 * 128
    return lead, ((lead, half), (lead + half, width - lead - half))


def fused_shards(anchor, momentum, change, adam_first, adam_second, attn_out, grad_out):
    groups, devices = lax.axis_size("replica"), lax.axis_size("fsdp")
    depth = devices // 2
    rows, width = change.shape[1:]
    tokens = attn_out.shape[1]
    cols = width // groups
    lead, cuts = plan(width)
    rest = width - lead
    pieces = len(cuts)
    scale = (tokens * devices) ** (-0.5)
    dma = pltpu.SemaphoreType.DMA
    vmem = pltpu.VMEM
    in_hbm = pl.BlockSpec(memory_space=pltpu.HBM)
    in_vmem = pl.BlockSpec(memory_space=pltpu.VMEM)
    summed, anchor_row, gradient, input_grad = pl.pallas_call(
        functools.partial(kernel, depth, groups, scale, lead, cuts),
        out_shape=(
            jax.ShapeDtypeStruct((rows, cols), f32),
            jax.ShapeDtypeStruct((rows, width), bf16),
            jax.ShapeDtypeStruct((rows, width), f32),
            jax.ShapeDtypeStruct((tokens, width), bf16),
        ),
        in_specs=[in_hbm] * 5,
        out_specs=(in_vmem,) * 4,
        scratch_shapes=[
            vmem((rows, cols), f32),
            vmem((rows, cols), f32),
            vmem((rows, width), f32),
            vmem((tokens, width), bf16),
            vmem((tokens, width), bf16),
            vmem((2 * rows, tokens), bf16),
            vmem((groups, rows, cols), bf16),
            vmem((groups - 1, rows, cols), bf16),
            vmem((depth, rows, width), f32),
            vmem((rows, width), f32),
            vmem((depth, rows, width), bf16),
            vmem((depth, rows, width), bf16),
            vmem((depth - 1, rows, width), bf16),
            vmem((depth + 1, rows, width), bf16),
            vmem((devices, rows, width), bf16),
            vmem((depth, 2 * rows, lead), f32),
            vmem((depth - 1, 2 * rows, lead), bf16),
            vmem((depth + 1, 2 * rows, lead), bf16),
            vmem((rows, lead), bf16),
            vmem((rows, lead), bf16),
            dma((5,)),
            dma((groups - 1,)), dma((groups - 1,)),
            dma((depth * pieces,)), dma((depth * pieces,)),
            dma((depth * pieces,)), dma(((depth + 1) * pieces,)),
            dma((depth - 1,)), dma((depth + 1,)), dma((1,)), dma((1,)),
            dma((5 * devices,)), dma((groups * devices,)),
        ],
        compiler_params=pltpu.CompilerParams(
            collective_id=0, has_side_effects=True, vmem_limit_bytes=38 * 2**20
        ),
    )(*(
        pltpu.with_memory_space_constraint(array, pltpu.HBM)
        for array in (anchor, momentum, change[0], attn_out[0], grad_out[0])
    ))
    lines = rows // 4
    block = jax.ShapeDtypeStruct((rows, width), f32)
    quarter = jax.ShapeDtypeStruct((rows, cols), f32)
    outs = pl.pallas_call(
        functools.partial(finish_kernel, groups, lines),
        out_shape=(
            quarter, quarter, block, block, block, jax.ShapeDtypeStruct((tokens, width), bf16),
        ),
        in_specs=[in_vmem] * 8,
        out_specs=(in_hbm,) * 6,
        scratch_shapes=[
            vmem((rows, cols), f32), vmem((rows, cols), f32),
            vmem((rows, width), f32), vmem((rows, width), f32), vmem((rows, width), f32),
            dma((3 * (rows // lines) + 3,)),
        ],
        compiler_params=pltpu.CompilerParams(vmem_limit_bytes=12 * 2**20),
    )(anchor, momentum, summed, anchor_row, adam_first[0], adam_second[0], gradient, input_grad)
    return (*outs[:2], *(out[None] for out in outs[2:]))


def shards(*arrays):
    groups, devices = lax.axis_size("replica"), lax.axis_size("fsdp")
    rows, width = arrays[2].shape[1:]
    fits = (
        groups == 4 and devices == 8 and rows % 32 == 0
        and (2 * rows) % 128 == 0 and width % (128 * groups) == 0
        and plan(width)[0] > 0
        and arrays[5].shape[1] * width <= 2**21
    )
    return (fused_shards if fits else plain_shards)(*arrays)


def solution(mesh):
    in_specs = (P("fsdp", "replica"),) * 2 + (P("replica", "fsdp", None),) * 5
    out_specs = (P("fsdp", "replica"),) * 2 + (P("replica", "fsdp", None),) * 4
    return jax.shard_map(shards, mesh=mesh, in_specs=in_specs, out_specs=out_specs, check_vma=False)
```

```python
import functools

import jax
import jax.numpy as jnp
from jax import lax
from jax.experimental import pallas as pl
from jax.experimental.pallas import tpu as pltpu
from jax.sharding import PartitionSpec as P

outer_rate = 0.7
outer_mu = 0.9
inner_rate = 0.005
beta_one = 0.9
beta_two = 0.95
decay_rate = 0.1
epsilon = 1e-08

MESH = pl.DeviceIdType.MESH
f32 = jnp.float32
bf16 = jnp.bfloat16


def adam(anchor_next, first, second, gradient):
    first_next = beta_one * first + (1.0 - beta_one) * gradient
    second_next = beta_two * second + (1.0 - beta_two) * gradient * gradient
    local = anchor_next - inner_rate * (
        first_next / (jnp.sqrt(second_next) + epsilon) + decay_rate * anchor_next
    )
    return local, first_next, second_next


def outer_step(anchor, momentum, summed, groups):
    outer_grad = -summed / groups
    new_momentum = outer_mu * momentum + outer_grad
    new_anchor = anchor - outer_rate * (outer_grad + outer_mu * new_momentum)
    return new_anchor, new_momentum


def plain_shards(anchor, momentum, change, adam_first, adam_second, attn_out, grad_out):
    groups = lax.axis_size("replica")
    summed = lax.psum_scatter(change[0], "replica", scatter_dimension=1, tiled=True)
    new_anchor, new_momentum = outer_step(anchor, momentum, summed, groups)
    anchor_next = lax.all_gather(new_anchor, "replica", axis=1, tiled=True)
    inputs, cotangent = attn_out[0], grad_out[0]
    grad_scale = (inputs.shape[0] * lax.axis_size("fsdp")) ** (-0.5)
    gradient = grad_scale * lax.psum_scatter(
        lax.dot_general(inputs, cotangent, (((0,), (0,)), ((), ())), preferred_element_type=f32),
        "fsdp",
        scatter_dimension=0,
        tiled=True,
    )
    input_grad = lax.dot_general(
        cotangent,
        lax.all_gather(anchor_next.astype(bf16), "fsdp", axis=0, tiled=True),
        (((1,), (1,)), ((), ())),
        preferred_element_type=f32,
    ).astype(bf16)
    local, first, second = adam(anchor_next, adam_first[0], adam_second[0], gradient)
    return new_anchor, new_momentum, local[None], first[None], second[None], input_grad[None]


INNER_STEPS = (
    "B00", "y00", "B0L", "B01", "B10", "B1L", "B11", "B20", "y01", "E0", "B2L", "B21", "B30", "L0", "B3L",
    "B31", "W", "own", "y11", "L2", "aa0", "ao1", "ac0", "L1", "ab0", "xo0", "S00", "y10", "ab1", "S01",
    "aa1", "xc0", "xa0", "ac1", "xo1", "y21", "xb0", "y31", "Mo", "S11", "xa1", "S20", "xb1", "y30", "S10",
    "CL", "Mb", "S21", "xc1", "Ma", "Mc", "F0", "F1", "FL",
)
OUTER_STEPS = (
    "B00", "y00", "B0L", "L0", "B01", "B10", "B1L", "B11", "B20", "L1", "B2L", "y01", "B21", "B30", "B3L",
    "B31", "W", "own", "yL", "S00", "y11", "y10", "y20", "S01", "ab0", "xo0", "L2", "ab1", "S11", "ad0",
    "CL", "S10", "y21", "ac0", "xb1", "S20", "xb0", "ac1", "C0", "FL", "ao1", "Mb", "xc1", "S21", "ad1",
    "y31", "xc0", "xd0", "xo1", "Mc", "xd1", "Mo", "F0", "Md", "F1",
)
ROUTES = {
    True: {"o0": "bayxs", "a0": "ybxs", "o1": "abxs", "a1": "axs", "c0": "yaxs"},
    False: {"o0": "bxs"},
}
LONE = {True: "axs", False: "xs"}


def kernel(
    depth, groups, scale, lead, cuts, extras,
    anchor_hbm, momentum_hbm, change_hbm, attn_hbm, cot_hbm,
    summed_ref, row_ref, grad_ref, back,
    anchor, momentum, change, attn, cot, flipped,
    part, got, own, other, psend, ry, zsend, chain, weights,
    lead_own, lead_send, lead_chain, lead_out, lead_in,
    local_sem, part_s, part_r, py_s, py_r, ch_s, ch_r,
    lz_s, lz_r, ly_s, ly_r, ag_s, ag_r,
):
    r = lax.axis_index("replica")
    f = lax.axis_index("fsdp")
    x, core = r // 2, r % 2
    z, y = f // 2, f % 2
    over_x, over_y = 1 - x, 1 - y
    rows, width = change.shape
    cols = width // groups
    pair = 2 * rows
    last = depth - 1
    pieces = len(cuts)
    inner = jnp.logical_and(z > 0, z < last)
    low = z < depth // 2
    inward = z + jnp.where(low, 1, -1)
    outward = z - jnp.where(low, 1, -1)
    places = {
        True: {"o": z, "a": outward, "b": inward, "c": last - outward},
        False: {"o": z, "b": inward, "c": last - inward, "d": last - z},
    }
    flip_y = {"replica": r, "fsdp": z * 2 + over_y}
    sibling = {"replica": x * 2 + (1 - core), "fsdp": f}
    to_inward = {"replica": r, "fsdp": inward * 2 + y}
    to_outward = {"replica": r, "fsdp": outward * 2 + y}
    links = {
        "a": to_outward, "b": to_inward, "y": flip_y, "s": sibling,
        "x": {"replica": over_x * 2 + core, "fsdp": f},
    }

    def block_at(i):
        lower = jnp.where(i < last - z, last - i, i - (last - z))
        upper = jnp.where(i < z, i, last - (i - z))
        return jnp.where(low, lower, upper)

    def block_columns(i):
        return pl.ds(pl.multiple_of(block_at(i) * pair, 128), pair)

    def piece(h):
        return pl.ds(*cuts[h]) if h < pieces else pl.ds(0, lead)

    loads = []

    def load(src, dst):
        loads.append(pltpu.make_async_copy(src, dst, local_sem.at[len(loads)]))
        loads[-1].start()
        return loads[-1]

    attn_in = [load(attn_hbm.at[:, block_columns(0)], attn.at[0])]
    cot_in = {0: load(cot_hbm.at[:, piece(0)], cot.at[:, piece(0)])}
    change_in = load(change_hbm, change)
    for h in (pieces, *range(1, pieces)):
        cot_in[h] = load(cot_hbm.at[:, piece(h)], cot.at[:, piece(h)])
    for i in range(1, depth):
        attn_in.append(load(attn_hbm.at[:, block_columns(i)], attn.at[i]))
    outer_in = (load(anchor_hbm, anchor), load(momentum_hbm, momentum))

    barrier = pltpu.get_barrier_semaphore()
    for k in range(1, groups):
        pl.semaphore_signal(
            barrier, inc=1, device_id={"replica": (r + k) % groups, "fsdp": f}, device_id_type=MESH
        )
    pl.semaphore_signal(barrier, inc=1, device_id=flip_y, device_id_type=MESH)
    pl.semaphore_signal(barrier, inc=1, device_id=to_inward, device_id_type=MESH)

    @pl.when(inner)
    def _():
        pl.semaphore_signal(barrier, inc=1, device_id=to_outward, device_id_type=MESH)

    def remote(src, dst, send, recv, device):
        return pltpu.make_async_remote_copy(
            src_ref=src, dst_ref=dst, send_sem=send, recv_sem=recv,
            device_id=device, device_id_type=MESH,
        )

    change_in.wait()
    for k in range(1, groups):
        at = pl.multiple_of(((r + k) % groups) * cols, 128)
        part[k] = change[:, pl.ds(at, cols)].astype(bf16)
    pl.semaphore_wait(barrier, groups + 1 + jnp.where(inner, 1, 0))
    parts = []
    for k in range(1, groups):
        parts.append(remote(
            part.at[k], got.at[k - 1], part_s.at[k - 1], part_r.at[k - 1],
            {"replica": (r + k) % groups, "fsdp": f},
        ))
        parts[-1].start()

    lines = 16

    def by_rows(body, count):
        def step(j, carry):
            body(pl.ds(pl.multiple_of(j * lines, lines), lines))
            return carry

        lax.fori_loop(0, count // lines, step, 0)

    def y_copy(i, h):
        return remote(
            psend.at[i, :, piece(h)], ry.at[i, :, piece(h)],
            py_s.at[(pieces + 1) * i + h], py_r.at[(pieces + 1) * i + h], flip_y,
        )

    def route(inside, i):
        if not inside:
            return i, to_inward
        return (depth - 1 + i, to_inward) if i < 2 else (depth - 1, to_outward)

    away = pl.multiple_of((1 - y) * rows, 16)
    home = pl.multiple_of(y * rows, 16)

    def lead_rows(ref, slot):
        return ref.at[slot, pl.ds(home, rows)] if slot == 2 else ref.at[slot]

    def lead_copy(inside, i):
        slot, device = route(inside, i)
        src = lead_send.at[i] if inside else lead_rows(lead_send, i)
        return remote(src, lead_rows(lead_chain, slot), lz_s.at[i], lz_r.at[slot], device)

    def z_copy(inside, i, h):
        slot, device = route(inside, i)
        return remote(
            zsend.at[i, :, piece(h)], chain.at[slot, :, piece(h)],
            ch_s.at[pieces * i + h], ch_r.at[pieces * slot + h], device,
        )

    def extra_copy(h):
        return remote(
            psend.at[2, :, piece(h)], chain.at[depth, :, piece(h)],
            ch_s.at[pieces * last + h], ch_r.at[pieces * depth + h], to_outward,
        )

    def lead_arrived(slot):
        ref = lead_rows(lead_chain, slot)
        remote(ref, ref, lz_s.at[0], lz_r.at[slot], flip_y).wait_recv()

    def z_arrived(slot, h):
        remote(
            zsend.at[0, :, piece(h)], chain.at[slot, :, piece(h)],
            ch_s.at[h], ch_r.at[pieces * slot + h], flip_y,
        ).wait_recv()

    sends = {True: [], False: []}

    def start(inside, make):
        make().start()
        sends[inside].append(make)

    def multiply(i, h):
        if h == 0:
            attn_in[i].wait()
            flipped[...] = attn[i].T
        if i == 0:
            cot_in[h].wait()
        product = jnp.dot(flipped[...], cot[:, piece(h)], preferred_element_type=f32)
        upper, lower = product[:rows], product[rows:]
        across = jnp.where(y == 0, lower, upper)
        if h < pieces or i == 2:
            psend[i, :, piece(h)] = across.astype(bf16)
        if h == pieces:
            lead_own[i] = product
            return
        own[i, :, piece(h)] = jnp.where(y == 0, upper, lower)
        if i == last and h < extras:
            other[:, piece(h)] = across

    def outer():
        for copy in outer_in:
            copy.wait()
        for copy in parts:
            copy.wait_recv()
        mine = pl.ds(pl.multiple_of(r * cols, 128), cols)
        total = change[:, mine]
        for k in range(1, groups):
            total = total + got[k - 1].astype(f32)
        summed_ref[...] = total
        weights[f, :, mine] = outer_step(anchor[...], momentum[...], total, groups)[0].astype(bf16)

    def shard_copy(where, index, device):
        zs, ys, xs, cs = where
        at = pl.multiple_of((xs * 2 + cs) * cols, 128)
        ref = weights.at[zs * 2 + ys, :, pl.ds(at, cols)]
        return remote(
            ref, ref, ag_s.at[index], ag_r.at[((zs * 2 + ys) * 2 + xs) * 2 + cs], device
        )

    def arrived(where):
        shard_copy(where, 0, sibling).wait_recv()

    used = {True: 0, False: 0}

    def spread(inside, where, names):
        for name in names:
            start(inside, functools.partial(shard_copy, where, used[inside], links[name]))
            used[inside] += 1

    def lead_step(inside, i):
        slot = i if i < 2 else depth - 1
        if inside:
            lead_arrived(slot)
        elif i == 2:
            y_copy(i, pieces).wait_recv()
            lead_send[i, pl.ds(home, rows)] = (
                lead_own[i, pl.ds(home, rows)] + ry[i, :, piece(pieces)].astype(f32)
            ).astype(bf16)
            start(inside, functools.partial(lead_copy, inside, i))
            return

        def add(there):
            value = lead_own[i, there]
            if inside:
                value = value + lead_chain[slot, there].astype(f32)
            lead_send[i, there] = value.astype(bf16)

        by_rows(add, pair)
        start(inside, functools.partial(lead_copy, inside, i))

    def chain_step(inside, i, h):
        crossed = not inside or i < 2 or h >= extras
        slot = i if i < 2 else depth - 1
        if crossed:
            y_copy(i, h).wait_recv()
        if inside:
            z_arrived(slot, h)

        def add(there):
            value = own[i, there, piece(h)]
            if crossed:
                value = value + ry[i, there, piece(h)].astype(f32)
            if inside:
                value = value + chain[slot, there, piece(h)].astype(f32)
            zsend[i, there, piece(h)] = value.astype(bf16)

        by_rows(add, rows)
        start(inside, functools.partial(z_copy, inside, i, h))

    def cross_step(h):
        z_arrived(depth, h)

        def add(there):
            psend[last, there, piece(h)] = (
                other[there, piece(h)] + chain[depth, there, piece(h)].astype(f32)
            ).astype(bf16)

        by_rows(add, rows)
        start(False, functools.partial(y_copy, last, h))

    ends = {True: (2, depth), False: (depth - 1,)}

    def lead_swap():
        return remote(lead_out, lead_in, ly_s.at[0], ly_r.at[0], flip_y)


    def cross_lead(inside):
        slot = ends[inside][-1]
        lead_arrived(slot)
        lead_out[...] = (
            lead_own[last, pl.ds(away, rows)] + lead_chain[slot, pl.ds(away, rows)].astype(f32)
        ).astype(bf16)
        start(inside, lead_swap)

    def finish_lead(inside):
        lead_swap().wait_recv()
        if inside:
            lead_arrived(2)
        value = lead_own[last, pl.ds(home, rows)] + lead_in[...].astype(f32)
        for slot in ends[inside]:
            value = value + lead_chain[slot, pl.ds(home, rows)].astype(f32)
        grad_ref[:, :lead] = value * scale

    def finish(inside, h):
        y_copy(last, h).wait_recv()
        for slot in ends[inside]:
            z_arrived(slot, h)

        def add(there):
            value = own[last, there, piece(h)] + ry[last, there, piece(h)].astype(f32)
            for slot in ends[inside]:
                value = value + chain[slot, there, piece(h)].astype(f32)
            grad_ref[there, piece(h)] = value * scale

        by_rows(add, rows)

    def take(inside, step):
        kind, spot = step[0], step[1:]
        if step == "own":
            spread(inside, (z, y, x, core), ROUTES[inside]["o0"])
        elif kind in "ax":
            zs, ys = places[inside][spot[0]], y if spot[1] == "0" else over_y
            if kind == "a":
                where = (zs, ys, x, core)
                arrived(where)
                spread(inside, where, ROUTES[inside].get(spot, LONE[inside]))
            else:
                where = (zs, ys, over_x, core)
                arrived(where)
                spread(inside, where, "s")
        elif kind == "L":
            lead_step(inside, int(spot))
        elif kind == "S":
            chain_step(inside, int(spot[0]), int(spot[1]))
        elif kind == "E":
            start(inside, functools.partial(extra_copy, int(spot)))
        elif kind == "y":
            i, h = (2, pieces) if step == "yL" else (int(spot[0]), int(spot[1]))
            start(inside, functools.partial(y_copy, i, h))
        elif step == "CL":
            cross_lead(inside)
        elif kind == "C":
            cross_step(int(spot))
        elif step == "FL":
            finish_lead(inside)
        elif kind == "F":
            finish(inside, int(spot))

    runs, joint = {True: [[]], False: [[]]}, {True: [], False: []}
    for inside, steps in ((True, INNER_STEPS), (False, OUTER_STEPS)):
        for step in steps:
            if step[0] in "BWM":
                joint[inside].append(step)
                runs[inside].append([])
            else:
                runs[inside][-1].append(step)

    for k in range(len(joint[True]) + 1):
        for inside in (True, False):
            if runs[inside][k]:
                @pl.when(inner if inside else jnp.logical_not(inner))
                def _():
                    for step in runs[inside][k]:
                        take(inside, step)

        if k == len(joint[True]):
            continue
        step = joint[True][k]
        if step[0] == "B":
            multiply(int(step[1]), pieces if step[2] == "L" else int(step[2]))
        elif step[0] == "W":
            outer()
        else:
            zs = jnp.where(inner, *(places[inside][joint[inside][k][1]] for inside in (True, False)))
            for ys in range(2):
                for xs in range(2):
                    arrived((zs, ys, xs, 1 - core))
            there = pl.ds(pl.multiple_of(zs * pair, 128), pair)
            block = weights[pl.ds(2 * zs, 2)].reshape(pair, width)
            back[:, there] = lax.dot_general(
                cot[...], block, (((1,), (1,)), ((), ())), preferred_element_type=f32
            ).astype(bf16)

    row_ref[...] = weights[f]
    for copy in parts:
        copy.wait_send()
    for inside in (True, False):
        @pl.when(inner if inside else jnp.logical_not(inner))
        def _():
            for make in sends[inside]:
                make().wait_send()


def finish_kernel(
    groups, lines,
    anchor, momentum, summed, row, first, second, gradient, back,
    anchor_hbm, momentum_hbm, local_hbm, first_hbm, second_hbm, back_hbm,
    anchor_out, momentum_out, local_out, first_out, second_out, sems,
):
    copies = []

    def put(src, dst):
        copies.append(pltpu.make_async_copy(src, dst, sems.at[len(copies)]))
        copies[-1].start()

    put(back, back_hbm)
    for k in range(row.shape[0] // lines):
        there = pl.ds(k * lines, lines)
        local, first_next, second_next = adam(
            row[there].astype(f32), first[there], second[there], gradient[there]
        )
        first_out[there] = first_next
        put(first_out.at[there], first_hbm.at[there])
        second_out[there] = second_next
        put(second_out.at[there], second_hbm.at[there])
        local_out[there] = local
        put(local_out.at[there], local_hbm.at[there])
    new_anchor, new_momentum = outer_step(anchor[...], momentum[...], summed[...], groups)
    anchor_out[...] = new_anchor
    put(anchor_out, anchor_hbm)
    momentum_out[...] = new_momentum
    put(momentum_out, momentum_hbm)
    for copy in copies:
        copy.wait()


def plan(width):
    lead = width // 6 // 128 * 128
    part = width // 2 // 128 * 128
    return lead, ((lead, part), (lead + part, width - lead - part)), 1


def fused_shards(anchor, momentum, change, adam_first, adam_second, attn_out, grad_out):
    groups, devices = lax.axis_size("replica"), lax.axis_size("fsdp")
    depth = devices // 2
    rows, width = change.shape[1:]
    tokens = attn_out.shape[1]
    cols = width // groups
    lead, cuts, extras = plan(width)
    rest = width - lead
    pieces = len(cuts)
    scale = (tokens * devices) ** (-0.5)
    dma = pltpu.SemaphoreType.DMA
    vmem = pltpu.VMEM
    in_hbm = pl.BlockSpec(memory_space=pltpu.HBM)
    in_vmem = pl.BlockSpec(memory_space=pltpu.VMEM)
    summed, anchor_row, gradient, input_grad = pl.pallas_call(
        functools.partial(kernel, depth, groups, scale, lead, cuts, extras),
        out_shape=(
            jax.ShapeDtypeStruct((rows, cols), f32),
            jax.ShapeDtypeStruct((rows, width), bf16),
            jax.ShapeDtypeStruct((rows, width), f32),
            jax.ShapeDtypeStruct((tokens, width), bf16),
        ),
        in_specs=[in_hbm] * 5,
        out_specs=(in_vmem,) * 4,
        scratch_shapes=[
            vmem((rows, cols), f32),
            vmem((rows, cols), f32),
            vmem((rows, width), f32),
            vmem((depth, tokens, 2 * rows), bf16),
            vmem((tokens, width), bf16),
            vmem((2 * rows, tokens), bf16),
            vmem((groups, rows, cols), bf16),
            vmem((groups - 1, rows, cols), bf16),
            vmem((depth, rows, width), f32),
            vmem((rows, width), f32),
            vmem((depth, rows, width), bf16),
            vmem((depth, rows, width), bf16),
            vmem((depth - 1, rows, width), bf16),
            vmem((depth + 1, rows, width), bf16),
            vmem((devices, rows, width), bf16),
            vmem((depth, 2 * rows, lead), f32),
            vmem((depth - 1, 2 * rows, lead), bf16),
            vmem((depth + 1, 2 * rows, lead), bf16),
            vmem((rows, lead), bf16),
            vmem((rows, lead), bf16),
            dma((depth + pieces + 4,)),
            dma((groups - 1,)), dma((groups - 1,)),
            dma((depth * (pieces + 1),)), dma((depth * (pieces + 1),)),
            dma((depth * pieces,)), dma(((depth + 1) * pieces,)),
            dma((depth - 1,)), dma((depth + 1,)), dma((1,)), dma((1,)),
            dma((5 * devices,)), dma((groups * devices,)),
        ],
        compiler_params=pltpu.CompilerParams(
            collective_id=0, has_side_effects=True, vmem_limit_bytes=38 * 2**20
        ),
    )(*(
        pltpu.with_memory_space_constraint(array, pltpu.HBM)
        for array in (anchor, momentum, change[0], attn_out[0], grad_out[0])
    ))
    lines = rows // 4
    block = jax.ShapeDtypeStruct((rows, width), f32)
    quarter = jax.ShapeDtypeStruct((rows, cols), f32)
    outs = pl.pallas_call(
        functools.partial(finish_kernel, groups, lines),
        out_shape=(
            quarter, quarter, block, block, block, jax.ShapeDtypeStruct((tokens, width), bf16),
        ),
        in_specs=[in_vmem] * 8,
        out_specs=(in_hbm,) * 6,
        scratch_shapes=[
            vmem((rows, cols), f32), vmem((rows, cols), f32),
            vmem((rows, width), f32), vmem((rows, width), f32), vmem((rows, width), f32),
            dma((3 * (rows // lines) + 3,)),
        ],
        compiler_params=pltpu.CompilerParams(vmem_limit_bytes=12 * 2**20),
    )(anchor, momentum, summed, anchor_row, adam_first[0], adam_second[0], gradient, input_grad)
    return (*outs[:2], *(out[None] for out in outs[2:]))


def shards(*arrays):
    groups, devices = lax.axis_size("replica"), lax.axis_size("fsdp")
    rows, width = arrays[2].shape[1:]
    fits = (
        groups == 4 and devices == 8 and rows % 32 == 0
        and (2 * rows) % 128 == 0 and width % (128 * groups) == 0
        and plan(width)[0] > 0
        and arrays[5].shape[1] * width <= 2**21
    )
    return (fused_shards if fits else plain_shards)(*arrays)


def solution(mesh):
    in_specs = (P("fsdp", "replica"),) * 2 + (P("replica", "fsdp", None),) * 5
    out_specs = (P("fsdp", "replica"),) * 2 + (P("replica", "fsdp", None),) * 4
    return jax.shard_map(shards, mesh=mesh, in_specs=in_specs, out_specs=out_specs, check_vma=False)
```

```python
import functools

import jax
import jax.numpy as jnp
from jax import lax
from jax.experimental import pallas as pl
from jax.experimental.pallas import tpu as pltpu
from jax.sharding import PartitionSpec as P

outer_rate = 0.7
outer_mu = 0.9
inner_rate = 0.005
beta_one = 0.9
beta_two = 0.95
decay_rate = 0.1
epsilon = 1e-08

MESH = pl.DeviceIdType.MESH
f32 = jnp.float32
bf16 = jnp.bfloat16


def adam(anchor_next, first, second, gradient):
    first_next = beta_one * first + (1.0 - beta_one) * gradient
    second_next = beta_two * second + (1.0 - beta_two) * gradient * gradient
    local = anchor_next - inner_rate * (
        first_next / (jnp.sqrt(second_next) + epsilon) + decay_rate * anchor_next
    )
    return local, first_next, second_next


def outer_step(anchor, momentum, summed, groups):
    outer_grad = -summed / groups
    new_momentum = outer_mu * momentum + outer_grad
    new_anchor = anchor - outer_rate * (outer_grad + outer_mu * new_momentum)
    return new_anchor, new_momentum


def plain_shards(anchor, momentum, change, adam_first, adam_second, attn_out, grad_out):
    groups = lax.axis_size("replica")
    summed = lax.psum_scatter(change[0], "replica", scatter_dimension=1, tiled=True)
    new_anchor, new_momentum = outer_step(anchor, momentum, summed, groups)
    anchor_next = lax.all_gather(new_anchor, "replica", axis=1, tiled=True)
    inputs, cotangent = attn_out[0], grad_out[0]
    grad_scale = (inputs.shape[0] * lax.axis_size("fsdp")) ** (-0.5)
    gradient = grad_scale * lax.psum_scatter(
        lax.dot_general(inputs, cotangent, (((0,), (0,)), ((), ())), preferred_element_type=f32),
        "fsdp",
        scatter_dimension=0,
        tiled=True,
    )
    input_grad = lax.dot_general(
        cotangent,
        lax.all_gather(anchor_next.astype(bf16), "fsdp", axis=0, tiled=True),
        (((1,), (1,)), ((), ())),
        preferred_element_type=f32,
    ).astype(bf16)
    local, first, second = adam(anchor_next, adam_first[0], adam_second[0], gradient)
    return new_anchor, new_momentum, local[None], first[None], second[None], input_grad[None]


INNER_STEPS = (
    "B00", "y00", "P", "B0L", "B01", "B10", "R", "E0", "B1L", "B11", "B20", "y01", "B2L", "B21", "B30",
    "L0", "B3L", "B31", "W", "own", "y11", "L2", "aa0", "ao1", "ac0", "L1", "ab0", "xo0", "S00", "y10",
    "ab1", "S01", "aa1", "xc0", "xa0", "ac1", "xo1", "y21", "xb0", "y31", "Mo", "S11", "xa1", "S20", "xb1",
    "y30", "CL", "Mb", "S10", "S21", "xc1", "Ma", "Mc", "F0", "F1", "FL",
)
OUTER_STEPS = (
    "B00", "y00", "P", "B0L", "L0", "B01", "B10", "R", "B1L", "B11", "B20", "L1", "B2L", "y01", "B21",
    "B30", "B3L", "B31", "W", "own", "S00", "y11", "y10", "y20", "S01", "L2", "ab0", "S11", "xo0", "ab1",
    "ad0", "CL", "S10", "y21", "ac0", "xb1", "S20", "xb0", "ac1", "C0", "FL", "ao1", "Mb", "xc1", "S21",
    "ad1", "y31", "xc0", "xd0", "xo1", "Mc", "xd1", "Mo", "F0", "Md", "F1",
)
ROUTES = {
    True: {"o0": "bayxs", "a0": "ybxs", "o1": "abxs", "a1": "axs", "c0": "yaxs"},
    False: {"o0": "bxs"},
}
LONE = {True: "axs", False: "xs"}


def kernel(
    depth, groups, scale, lead, cuts, extras,
    anchor_hbm, momentum_hbm, change_hbm, attn_hbm, cot_hbm,
    summed_ref, row_ref, grad_ref, back,
    anchor, momentum, change, attn, cot, flipped,
    part, got, own, other, psend, ry, zsend, chain, weights,
    lead_own, lead_send, lead_chain, lead_out, lead_in,
    local_sem, part_s, part_r, py_s, py_r, ch_s, ch_r,
    lz_s, lz_r, ly_s, ly_r, ag_s, ag_r,
):
    r = lax.axis_index("replica")
    f = lax.axis_index("fsdp")
    x, core = r // 2, r % 2
    z, y = f // 2, f % 2
    over_x, over_y = 1 - x, 1 - y
    rows, width = change.shape
    cols = width // groups
    pair = 2 * rows
    last = depth - 1
    pieces = len(cuts)
    inner = jnp.logical_and(z > 0, z < last)
    low = z < depth // 2
    inward = z + jnp.where(low, 1, -1)
    outward = z - jnp.where(low, 1, -1)
    places = {
        True: {"o": z, "a": outward, "b": inward, "c": last - outward},
        False: {"o": z, "b": inward, "c": last - inward, "d": last - z},
    }
    flip_y = {"replica": r, "fsdp": z * 2 + over_y}
    sibling = {"replica": x * 2 + (1 - core), "fsdp": f}
    to_inward = {"replica": r, "fsdp": inward * 2 + y}
    to_outward = {"replica": r, "fsdp": outward * 2 + y}
    links = {
        "a": to_outward, "b": to_inward, "y": flip_y, "s": sibling,
        "x": {"replica": over_x * 2 + core, "fsdp": f},
    }

    def block_at(i):
        lower = jnp.where(i < last - z, last - i, i - (last - z))
        upper = jnp.where(i < z, i, last - (i - z))
        return jnp.where(low, lower, upper)

    def block_order(k):
        return jnp.where(inner, 3 - k, k) if 0 < k < last else k

    def block_columns(k):
        return pl.ds(pl.multiple_of(block_at(block_order(k)) * pair, 128), pair)

    def piece(h):
        return pl.ds(*cuts[h]) if h < pieces else pl.ds(0, lead)

    loads = []

    def load(src, dst):
        loads.append(pltpu.make_async_copy(src, dst, local_sem.at[len(loads)]))
        loads[-1].start()
        return loads[-1]

    attn_in = [load(attn_hbm.at[:, block_columns(0)], attn.at[0])]
    cot_in = {0: load(cot_hbm.at[:, piece(0)], cot.at[:, piece(0)])}
    change_in = load(change_hbm, change)
    for h in (pieces, *range(1, pieces)):
        cot_in[h] = load(cot_hbm.at[:, piece(h)], cot.at[:, piece(h)])
    for i in range(1, depth):
        attn_in.append(load(attn_hbm.at[:, block_columns(i)], attn.at[i]))
    outer_in = (load(anchor_hbm, anchor), load(momentum_hbm, momentum))

    barrier = pltpu.get_barrier_semaphore()
    for k in range(1, groups):
        pl.semaphore_signal(
            barrier, inc=1, device_id={"replica": (r + k) % groups, "fsdp": f}, device_id_type=MESH
        )
    pl.semaphore_signal(barrier, inc=1, device_id=flip_y, device_id_type=MESH)
    pl.semaphore_signal(barrier, inc=1, device_id=to_inward, device_id_type=MESH)

    @pl.when(inner)
    def _():
        pl.semaphore_signal(barrier, inc=1, device_id=to_outward, device_id_type=MESH)

    def remote(src, dst, send, recv, device):
        return pltpu.make_async_remote_copy(
            src_ref=src, dst_ref=dst, send_sem=send, recv_sem=recv,
            device_id=device, device_id_type=MESH,
        )

    def quarter(xs, cs):
        return pl.ds(pl.multiple_of((xs * 2 + cs) * cols, 128), cols)

    def part_copy(k):
        return remote(
            part.at[k], got.at[k], part_s.at[k], part_r.at[k], links["s" if k < 2 else "x"]
        )

    def send_parts():
        change_in.wait()
        for k, xs in ((1, over_x), (0, x)):
            part[k] = change[:, quarter(xs, 1 - core)].astype(bf16)
            part_copy(k).start()

    def relay_parts():
        part_copy(1).wait_recv()
        part[2] = (change[:, quarter(over_x, core)] + got[1].astype(f32)).astype(bf16)
        part_copy(2).start()

    lines = 16

    def by_rows(body, count):
        def step(j, carry):
            body(pl.ds(pl.multiple_of(j * lines, lines), lines))
            return carry

        lax.fori_loop(0, count // lines, step, 0)

    def y_copy(i, h):
        return remote(
            psend.at[i, :, piece(h)], ry.at[i, :, piece(h)],
            py_s.at[pieces * i + h], py_r.at[pieces * i + h], flip_y,
        )

    def route(inside, i):
        if not inside:
            return i, to_inward
        return (depth - 1 + i, to_inward) if i < 2 else (depth - 1, to_outward)

    away = pl.multiple_of((1 - y) * rows, 16)
    home = pl.multiple_of(y * rows, 16)

    def lead_copy(inside, i):
        slot, device = route(inside, i)
        return remote(lead_send.at[i], lead_chain.at[slot], lz_s.at[i], lz_r.at[slot], device)

    def z_copy(inside, i, h):
        slot, device = route(inside, i)
        return remote(
            zsend.at[i, :, piece(h)], chain.at[slot, :, piece(h)],
            ch_s.at[pieces * i + h], ch_r.at[pieces * slot + h], device,
        )

    def extra_copy(h):
        return remote(
            psend.at[2, :, piece(h)], chain.at[depth, :, piece(h)],
            ch_s.at[pieces * last + h], ch_r.at[pieces * depth + h], to_outward,
        )

    def lead_arrived(slot):
        ref = lead_chain.at[slot]
        remote(ref, ref, lz_s.at[0], lz_r.at[slot], flip_y).wait_recv()

    def z_arrived(slot, h):
        remote(
            zsend.at[0, :, piece(h)], chain.at[slot, :, piece(h)],
            ch_s.at[h], ch_r.at[pieces * slot + h], flip_y,
        ).wait_recv()

    sends = {True: [], False: []}

    def start(inside, make):
        make().start()
        sends[inside].append(make)

    def multiply(k, h):
        i = block_order(k)
        if h == 0:
            attn_in[k].wait()
            flipped[...] = attn[k].T
        if k == 0:
            cot_in[h].wait()
        product = jnp.dot(flipped[...], cot[:, piece(h)], preferred_element_type=f32)
        if h == pieces:
            lead_own[i] = product
            return
        upper, lower = product[:rows], product[rows:]
        across = jnp.where(y == 0, lower, upper)
        psend[i, :, piece(h)] = across.astype(bf16)
        own[i, :, piece(h)] = jnp.where(y == 0, upper, lower)
        if k == last and h < extras:
            other[:, piece(h)] = across

    def outer():
        for copy in outer_in:
            copy.wait()
        mine = quarter(x, core)
        part_copy(0).wait_recv()
        part_copy(2).wait_recv()
        total = change[:, mine] + got[0].astype(f32) + got[2].astype(f32)
        summed_ref[...] = total
        weights[f, :, mine] = outer_step(anchor[...], momentum[...], total, groups)[0].astype(bf16)

    def shard_copy(where, index, device):
        zs, ys, xs, cs = where
        at = pl.multiple_of((xs * 2 + cs) * cols, 128)
        ref = weights.at[zs * 2 + ys, :, pl.ds(at, cols)]
        return remote(
            ref, ref, ag_s.at[index], ag_r.at[((zs * 2 + ys) * 2 + xs) * 2 + cs], device
        )

    def arrived(where):
        shard_copy(where, 0, sibling).wait_recv()

    used = {True: 0, False: 0}

    def spread(inside, where, names):
        for name in names:
            start(inside, functools.partial(shard_copy, where, used[inside], links[name]))
            used[inside] += 1

    def lead_step(inside, i):
        slot = i if i < 2 else depth - 1
        if inside:
            lead_arrived(slot)

        def add(there):
            value = lead_own[i, there]
            if inside:
                value = value + lead_chain[slot, there].astype(f32)
            lead_send[i, there] = value.astype(bf16)

        by_rows(add, pair)
        start(inside, functools.partial(lead_copy, inside, i))

    def chain_step(inside, i, h):
        crossed = not inside or i < 2 or h >= extras
        slot = i if i < 2 else depth - 1
        if crossed:
            y_copy(i, h).wait_recv()
        if inside:
            z_arrived(slot, h)

        def add(there):
            value = own[i, there, piece(h)]
            if crossed:
                value = value + ry[i, there, piece(h)].astype(f32)
            if inside:
                value = value + chain[slot, there, piece(h)].astype(f32)
            zsend[i, there, piece(h)] = value.astype(bf16)

        by_rows(add, rows)
        start(inside, functools.partial(z_copy, inside, i, h))

    def cross_step(h):
        z_arrived(depth, h)

        def add(there):
            psend[last, there, piece(h)] = (
                other[there, piece(h)] + chain[depth, there, piece(h)].astype(f32)
            ).astype(bf16)

        by_rows(add, rows)
        start(False, functools.partial(y_copy, last, h))

    ends = {True: (2, depth), False: (depth - 1,)}

    def lead_swap():
        return remote(lead_out, lead_in, ly_s.at[0], ly_r.at[0], flip_y)


    def cross_lead(inside):
        value = lead_own[last, pl.ds(away, rows)]
        for slot in ends[inside]:
            lead_arrived(slot)
            value = value + lead_chain[slot, pl.ds(away, rows)].astype(f32)
        lead_out[...] = value.astype(bf16)
        start(inside, lead_swap)

    def finish_lead(inside):
        lead_swap().wait_recv()
        value = lead_own[last, pl.ds(home, rows)] + lead_in[...].astype(f32)
        for slot in ends[inside]:
            value = value + lead_chain[slot, pl.ds(home, rows)].astype(f32)
        grad_ref[:, :lead] = value * scale

    def finish(inside, h):
        y_copy(last, h).wait_recv()
        for slot in ends[inside]:
            z_arrived(slot, h)

        def add(there):
            value = own[last, there, piece(h)] + ry[last, there, piece(h)].astype(f32)
            for slot in ends[inside]:
                value = value + chain[slot, there, piece(h)].astype(f32)
            grad_ref[there, piece(h)] = value * scale

        by_rows(add, rows)

    def take(inside, step):
        kind, spot = step[0], step[1:]
        if step == "own":
            spread(inside, (z, y, x, core), ROUTES[inside]["o0"])
        elif kind in "ax":
            zs, ys = places[inside][spot[0]], y if spot[1] == "0" else over_y
            if kind == "a":
                where = (zs, ys, x, core)
                arrived(where)
                spread(inside, where, ROUTES[inside].get(spot, LONE[inside]))
            else:
                where = (zs, ys, over_x, core)
                arrived(where)
                spread(inside, where, "s")
        elif kind == "L":
            lead_step(inside, int(spot))
        elif kind == "S":
            chain_step(inside, int(spot[0]), int(spot[1]))
        elif kind == "E":
            start(inside, functools.partial(extra_copy, int(spot)))
        elif kind == "y":
            start(inside, functools.partial(y_copy, int(spot[0]), int(spot[1])))
        elif step == "CL":
            cross_lead(inside)
        elif kind == "C":
            cross_step(int(spot))
        elif step == "FL":
            finish_lead(inside)
        elif kind == "F":
            finish(inside, int(spot))

    runs, joint = {True: [[]], False: [[]]}, {True: [], False: []}
    for inside, steps in ((True, INNER_STEPS), (False, OUTER_STEPS)):
        for step in steps:
            if step[0] in "BPRWM":
                joint[inside].append(step)
                runs[inside].append([])
            else:
                runs[inside][-1].append(step)

    for k in range(len(joint[True]) + 1):
        for inside in (True, False):
            if runs[inside][k]:
                @pl.when(inner if inside else jnp.logical_not(inner))
                def _():
                    for step in runs[inside][k]:
                        take(inside, step)

        if k == len(joint[True]):
            continue
        step = joint[True][k]
        if step[0] == "B":
            multiply(int(step[1]), pieces if step[2] == "L" else int(step[2]))
            if step == "B00":
                pl.semaphore_wait(barrier, groups + 1 + jnp.where(inner, 1, 0))
        elif step[0] == "P":
            send_parts()
        elif step[0] == "R":
            relay_parts()
        elif step[0] == "W":
            outer()
        else:
            zs = jnp.where(inner, *(places[inside][joint[inside][k][1]] for inside in (True, False)))
            for ys in range(2):
                for xs in range(2):
                    arrived((zs, ys, xs, 1 - core))
            if k == len(joint[True]) - 1:
                row_ref[...] = weights[f]
            there = pl.ds(pl.multiple_of(zs * pair, 128), pair)
            block = weights[pl.ds(2 * zs, 2)].reshape(pair, width)
            back[:, there] = lax.dot_general(
                cot[...], block, (((1,), (1,)), ((), ())), preferred_element_type=f32
            ).astype(bf16)

    for k in range(3):
        part_copy(k).wait_send()
    for inside in (True, False):
        @pl.when(inner if inside else jnp.logical_not(inner))
        def _():
            for make in sends[inside]:
                make().wait_send()


def finish_kernel(
    groups, lines,
    anchor, momentum, summed, row, first, second, gradient, back,
    anchor_hbm, momentum_hbm, local_hbm, first_hbm, second_hbm, back_hbm,
    anchor_out, momentum_out, local_out, first_out, second_out, sems,
):
    copies = []

    def put(src, dst):
        copies.append(pltpu.make_async_copy(src, dst, sems.at[len(copies)]))
        copies[-1].start()

    put(back, back_hbm)
    for k in range(row.shape[0] // lines):
        there = pl.ds(k * lines, lines)
        local, first_next, second_next = adam(
            row[there].astype(f32), first[there], second[there], gradient[there]
        )
        first_out[there] = first_next
        put(first_out.at[there], first_hbm.at[there])
        second_out[there] = second_next
        put(second_out.at[there], second_hbm.at[there])
        local_out[there] = local
        put(local_out.at[there], local_hbm.at[there])
    new_anchor, new_momentum = outer_step(anchor[...], momentum[...], summed[...], groups)
    anchor_out[...] = new_anchor
    put(anchor_out, anchor_hbm)
    momentum_out[...] = new_momentum
    put(momentum_out, momentum_hbm)
    for copy in copies:
        copy.wait()


def plan(width):
    lead = width // 6 // 128 * 128
    part = width // 2 // 128 * 128
    return lead, ((lead, part), (lead + part, width - lead - part)), 1


def fused_shards(anchor, momentum, change, adam_first, adam_second, attn_out, grad_out):
    groups, devices = lax.axis_size("replica"), lax.axis_size("fsdp")
    depth = devices // 2
    rows, width = change.shape[1:]
    tokens = attn_out.shape[1]
    cols = width // groups
    lead, cuts, extras = plan(width)
    rest = width - lead
    pieces = len(cuts)
    scale = (tokens * devices) ** (-0.5)
    dma = pltpu.SemaphoreType.DMA
    vmem = pltpu.VMEM
    in_hbm = pl.BlockSpec(memory_space=pltpu.HBM)
    in_vmem = pl.BlockSpec(memory_space=pltpu.VMEM)
    summed, anchor_row, gradient, input_grad = pl.pallas_call(
        functools.partial(kernel, depth, groups, scale, lead, cuts, extras),
        out_shape=(
            jax.ShapeDtypeStruct((rows, cols), f32),
            jax.ShapeDtypeStruct((rows, width), bf16),
            jax.ShapeDtypeStruct((rows, width), f32),
            jax.ShapeDtypeStruct((tokens, width), bf16),
        ),
        in_specs=[in_hbm] * 5,
        out_specs=(in_vmem,) * 4,
        scratch_shapes=[
            vmem((rows, cols), f32),
            vmem((rows, cols), f32),
            vmem((rows, width), f32),
            vmem((depth, tokens, 2 * rows), bf16),
            vmem((tokens, width), bf16),
            vmem((2 * rows, tokens), bf16),
            vmem((3, rows, cols), bf16),
            vmem((3, rows, cols), bf16),
            vmem((depth, rows, width), f32),
            vmem((rows, width), f32),
            vmem((depth, rows, width), bf16),
            vmem((depth, rows, width), bf16),
            vmem((depth - 1, rows, width), bf16),
            vmem((depth + 1, rows, width), bf16),
            vmem((devices, rows, width), bf16),
            vmem((depth, 2 * rows, lead), f32),
            vmem((depth - 1, 2 * rows, lead), bf16),
            vmem((depth + 1, 2 * rows, lead), bf16),
            vmem((rows, lead), bf16),
            vmem((rows, lead), bf16),
            dma((depth + pieces + 4,)),
            dma((3,)), dma((3,)),
            dma((depth * pieces,)), dma((depth * pieces,)),
            dma((depth * pieces,)), dma(((depth + 1) * pieces,)),
            dma((depth - 1,)), dma((depth + 1,)), dma((1,)), dma((1,)),
            dma((5 * devices,)), dma((groups * devices,)),
        ],
        compiler_params=pltpu.CompilerParams(
            collective_id=0, has_side_effects=True, vmem_limit_bytes=38 * 2**20
        ),
    )(*(
        pltpu.with_memory_space_constraint(array, pltpu.HBM)
        for array in (anchor, momentum, change[0], attn_out[0], grad_out[0])
    ))
    lines = rows // 4
    block = jax.ShapeDtypeStruct((rows, width), f32)
    quarter = jax.ShapeDtypeStruct((rows, cols), f32)
    outs = pl.pallas_call(
        functools.partial(finish_kernel, groups, lines),
        out_shape=(
            quarter, quarter, block, block, block, jax.ShapeDtypeStruct((tokens, width), bf16),
        ),
        in_specs=[in_vmem] * 8,
        out_specs=(in_hbm,) * 6,
        scratch_shapes=[
            vmem((rows, cols), f32), vmem((rows, cols), f32),
            vmem((rows, width), f32), vmem((rows, width), f32), vmem((rows, width), f32),
            dma((3 * (rows // lines) + 3,)),
        ],
        compiler_params=pltpu.CompilerParams(vmem_limit_bytes=12 * 2**20),
    )(anchor, momentum, summed, anchor_row, adam_first[0], adam_second[0], gradient, input_grad)
    return (*outs[:2], *(out[None] for out in outs[2:]))


def shards(*arrays):
    groups, devices = lax.axis_size("replica"), lax.axis_size("fsdp")
    rows, width = arrays[2].shape[1:]
    fits = (
        groups == 4 and devices == 8 and rows % 32 == 0
        and (2 * rows) % 128 == 0 and width % (128 * groups) == 0
        and plan(width)[0] > 0
        and arrays[5].shape[1] * width <= 2**21
    )
    return (fused_shards if fits else plain_shards)(*arrays)


def solution(mesh):
    in_specs = (P("fsdp", "replica"),) * 2 + (P("replica", "fsdp", None),) * 5
    out_specs = (P("fsdp", "replica"),) * 2 + (P("replica", "fsdp", None),) * 4
    return jax.shard_map(shards, mesh=mesh, in_specs=in_specs, out_specs=out_specs, check_vma=False)
```

```python
import functools

import jax
import jax.numpy as jnp
from jax import lax
from jax.experimental import pallas as pl
from jax.experimental.pallas import tpu as pltpu
from jax.sharding import PartitionSpec as P

outer_rate = 0.7
outer_mu = 0.9
inner_rate = 0.005
beta_one = 0.9
beta_two = 0.95
decay_rate = 0.1
epsilon = 1e-08

MESH = pl.DeviceIdType.MESH
f32 = jnp.float32
bf16 = jnp.bfloat16


def adam(anchor_next, first, second, gradient):
    first_next = beta_one * first + (1.0 - beta_one) * gradient
    second_next = beta_two * second + (1.0 - beta_two) * gradient * gradient
    local = anchor_next - inner_rate * (
        first_next / (jnp.sqrt(second_next) + epsilon) + decay_rate * anchor_next
    )
    return local, first_next, second_next


def outer_step(anchor, momentum, summed, groups):
    outer_grad = -summed / groups
    new_momentum = outer_mu * momentum + outer_grad
    new_anchor = anchor - outer_rate * (outer_grad + outer_mu * new_momentum)
    return new_anchor, new_momentum


def plain_shards(anchor, momentum, change, adam_first, adam_second, attn_out, grad_out):
    groups = lax.axis_size("replica")
    summed = lax.psum_scatter(change[0], "replica", scatter_dimension=1, tiled=True)
    new_anchor, new_momentum = outer_step(anchor, momentum, summed, groups)
    anchor_next = lax.all_gather(new_anchor, "replica", axis=1, tiled=True)
    inputs, cotangent = attn_out[0], grad_out[0]
    grad_scale = (inputs.shape[0] * lax.axis_size("fsdp")) ** (-0.5)
    gradient = grad_scale * lax.psum_scatter(
        lax.dot_general(inputs, cotangent, (((0,), (0,)), ((), ())), preferred_element_type=f32),
        "fsdp",
        scatter_dimension=0,
        tiled=True,
    )
    input_grad = lax.dot_general(
        cotangent,
        lax.all_gather(anchor_next.astype(bf16), "fsdp", axis=0, tiled=True),
        (((1,), (1,)), ((), ())),
        preferred_element_type=f32,
    ).astype(bf16)
    local, first, second = adam(anchor_next, adam_first[0], adam_second[0], gradient)
    return new_anchor, new_momentum, local[None], first[None], second[None], input_grad[None]


INNER_STEPS = (
    "B00", "y00", "P", "B0L", "B01", "B10", "R", "E0", "B1L", "B11", "B20", "y01", "B2L", "B21", "B30",
    "L0", "B3L", "B31", "W", "own", "y11", "L2", "aa0", "ao1", "ac0", "L1", "ab0", "xo0", "S00", "y10",
    "ab1", "S01", "aa1", "xc0", "xa0", "ac1", "xo1", "y21", "xb0", "y31", "Mo", "S11", "xa1", "S20", "xb1",
    "y30", "CL", "Mb", "S10", "S21", "xc1", "Ma", "Mc", "F0", "F1", "FL",
)
OUTER_STEPS = (
    "B00", "y00", "P", "B0L", "L0", "B01", "B10", "R", "B1L", "B11", "B20", "L1", "B2L", "y01", "B21",
    "B30", "B3L", "B31", "W", "own", "S00", "y11", "y10", "y20", "S01", "L2", "ab0", "S11", "xo0", "ab1",
    "ad0", "CL", "S10", "y21", "ac0", "xb1", "S20", "xb0", "ac1", "C0", "FL", "ao1", "Mb", "xc1", "S21",
    "ad1", "y31", "xc0", "xd0", "xo1", "Mc", "xd1", "Mo", "F0", "Md", "F1",
)
ROUTES = {
    True: {"o0": "bayxs", "a0": "ybxs", "o1": "abxs", "a1": "axs", "c0": "yaxs"},
    False: {"o0": "bxs"},
}
LONE = {True: "axs", False: "xs"}


def kernel(
    depth, groups, scale, lead, cuts, extras,
    anchor_hbm, momentum_hbm, change_hbm, attn_hbm, cot_hbm,
    summed_ref, row_ref, grad_ref, back,
    anchor, momentum, change, attn, cot, flipped,
    part, got, own, other, psend, ry, zsend, chain, weights,
    lead_own, lead_send, lead_chain, lead_out, lead_in,
    local_sem, part_s, part_r, py_s, py_r, ch_s, ch_r,
    lz_s, lz_r, ly_s, ly_r, ag_s, ag_r,
):
    r = lax.axis_index("replica")
    f = lax.axis_index("fsdp")
    x, core = r // 2, r % 2
    z, y = f // 2, f % 2
    over_x, over_y = 1 - x, 1 - y
    rows, width = change.shape
    cols = width // groups
    pair = 2 * rows
    last = depth - 1
    pieces = len(cuts)
    inner = jnp.logical_and(z > 0, z < last)
    low = z < depth // 2
    inward = z + jnp.where(low, 1, -1)
    outward = z - jnp.where(low, 1, -1)
    places = {
        True: {"o": z, "a": outward, "b": inward, "c": last - outward},
        False: {"o": z, "b": inward, "c": last - inward, "d": last - z},
    }
    flip_y = {"replica": r, "fsdp": z * 2 + over_y}
    sibling = {"replica": x * 2 + (1 - core), "fsdp": f}
    to_inward = {"replica": r, "fsdp": inward * 2 + y}
    to_outward = {"replica": r, "fsdp": outward * 2 + y}
    links = {
        "a": to_outward, "b": to_inward, "y": flip_y, "s": sibling,
        "x": {"replica": over_x * 2 + core, "fsdp": f},
    }

    def block_at(i):
        lower = jnp.where(i < last - z, last - i, i - (last - z))
        upper = jnp.where(i < z, i, last - (i - z))
        return jnp.where(low, lower, upper)

    def block_order(k):
        return jnp.where(inner, 3 - k, k) if 0 < k < last else k

    def block_columns(k):
        return pl.ds(pl.multiple_of(block_at(block_order(k)) * pair, 128), pair)

    def piece(h):
        return pl.ds(*cuts[h]) if h < pieces else pl.ds(0, lead)

    loads = []

    def load(src, dst):
        loads.append(pltpu.make_async_copy(src, dst, local_sem.at[len(loads)]))
        loads[-1].start()
        return loads[-1]

    attn_in = [load(attn_hbm.at[:, block_columns(0)], attn.at[0])]
    cot_in = {0: load(cot_hbm.at[:, piece(0)], cot.at[:, piece(0)])}
    change_in = load(change_hbm, change)
    for h in (pieces, *range(1, pieces)):
        cot_in[h] = load(cot_hbm.at[:, piece(h)], cot.at[:, piece(h)])
    for i in range(1, depth):
        attn_in.append(load(attn_hbm.at[:, block_columns(i)], attn.at[i]))
    outer_in = (load(anchor_hbm, anchor), load(momentum_hbm, momentum))

    barrier = pltpu.get_barrier_semaphore()
    for name in "sxyb":
        pl.semaphore_signal(barrier, inc=1, device_id=links[name], device_id_type=MESH)

    @pl.when(inner)
    def _():
        pl.semaphore_signal(barrier, inc=1, device_id=to_outward, device_id_type=MESH)

    def remote(src, dst, send, recv, device):
        return pltpu.make_async_remote_copy(
            src_ref=src, dst_ref=dst, send_sem=send, recv_sem=recv,
            device_id=device, device_id_type=MESH,
        )

    def quarter(xs, cs):
        return pl.ds(pl.multiple_of((xs * 2 + cs) * cols, 128), cols)

    def part_copy(k):
        return remote(
            part.at[k], got.at[k], part_s.at[k], part_r.at[k], links["s" if k < 2 else "x"]
        )

    def send_parts():
        change_in.wait()
        for k, xs in ((1, over_x), (0, x)):
            part[k] = change[:, quarter(xs, 1 - core)].astype(bf16)
            part_copy(k).start()

    def relay_parts():
        part_copy(1).wait_recv()
        part[2] = (change[:, quarter(over_x, core)] + got[1].astype(f32)).astype(bf16)
        part_copy(2).start()

    lines = 32

    def by_rows(body, count):
        def step(j, carry):
            body(pl.ds(pl.multiple_of(j * lines, lines), lines))
            return carry

        lax.fori_loop(0, count // lines, step, 0)

    def y_copy(i, h):
        return remote(
            psend.at[i, :, piece(h)], ry.at[i, :, piece(h)],
            py_s.at[pieces * i + h], py_r.at[pieces * i + h], flip_y,
        )

    def route(inside, i):
        if not inside:
            return i, to_inward
        return (depth - 1 + i, to_inward) if i < 2 else (depth - 1, to_outward)

    away = pl.multiple_of((1 - y) * rows, 16)
    home = pl.multiple_of(y * rows, 16)

    def lead_copy(inside, i):
        slot, device = route(inside, i)
        return remote(lead_send.at[i], lead_chain.at[slot], lz_s.at[i], lz_r.at[slot], device)

    def z_copy(inside, i, h):
        slot, device = route(inside, i)
        return remote(
            zsend.at[i, :, piece(h)], chain.at[slot, :, piece(h)],
            ch_s.at[pieces * i + h], ch_r.at[pieces * slot + h], device,
        )

    def extra_copy(h):
        return remote(
            psend.at[2, :, piece(h)], chain.at[depth, :, piece(h)],
            ch_s.at[pieces * last + h], ch_r.at[pieces * depth + h], to_outward,
        )

    def lead_arrived(slot):
        ref = lead_chain.at[slot]
        remote(ref, ref, lz_s.at[0], lz_r.at[slot], flip_y).wait_recv()

    def z_arrived(slot, h):
        remote(
            zsend.at[0, :, piece(h)], chain.at[slot, :, piece(h)],
            ch_s.at[h], ch_r.at[pieces * slot + h], flip_y,
        ).wait_recv()

    sends = {True: [], False: []}

    def start(inside, make):
        make().start()
        sends[inside].append(make)

    def multiply(k, h):
        i = block_order(k)
        if h == 0:
            attn_in[k].wait()
            flipped[...] = attn[k].T
        if k == 0:
            cot_in[h].wait()
        product = jnp.dot(flipped[...], cot[:, piece(h)], preferred_element_type=f32)
        if h == pieces:
            lead_own[i] = product
            return
        upper, lower = product[:rows], product[rows:]
        across = jnp.where(y == 0, lower, upper)
        psend[i, :, piece(h)] = across.astype(bf16)
        own[i, :, piece(h)] = jnp.where(y == 0, upper, lower)
        if k == last and h < extras:
            other[:, piece(h)] = across

    def outer():
        for copy in outer_in:
            copy.wait()
        mine = quarter(x, core)
        part_copy(0).wait_recv()
        part_copy(2).wait_recv()
        total = change[:, mine] + got[0].astype(f32) + got[2].astype(f32)
        summed_ref[...] = total
        weights[f, :, mine] = outer_step(anchor[...], momentum[...], total, groups)[0].astype(bf16)

    def shard_copy(where, index, device):
        zs, ys, xs, cs = where
        at = pl.multiple_of((xs * 2 + cs) * cols, 128)
        ref = weights.at[zs * 2 + ys, :, pl.ds(at, cols)]
        return remote(
            ref, ref, ag_s.at[index], ag_r.at[((zs * 2 + ys) * 2 + xs) * 2 + cs], device
        )

    def arrived(where):
        shard_copy(where, 0, sibling).wait_recv()

    used = {True: 0, False: 0}

    def spread(inside, where, names):
        for name in names:
            start(inside, functools.partial(shard_copy, where, used[inside], links[name]))
            used[inside] += 1

    def lead_step(inside, i):
        slot = i if i < 2 else depth - 1
        if inside:
            lead_arrived(slot)

        def add(there):
            value = lead_own[i, there]
            if inside:
                value = value + lead_chain[slot, there].astype(f32)
            lead_send[i, there] = value.astype(bf16)

        by_rows(add, pair)
        start(inside, functools.partial(lead_copy, inside, i))

    def chain_step(inside, i, h):
        crossed = not inside or i < 2 or h >= extras
        slot = i if i < 2 else depth - 1
        if crossed:
            y_copy(i, h).wait_recv()
        if inside:
            z_arrived(slot, h)

        def add(there):
            value = own[i, there, piece(h)]
            if crossed:
                value = value + ry[i, there, piece(h)].astype(f32)
            if inside:
                value = value + chain[slot, there, piece(h)].astype(f32)
            zsend[i, there, piece(h)] = value.astype(bf16)

        by_rows(add, rows)
        start(inside, functools.partial(z_copy, inside, i, h))

    def cross_step(h):
        z_arrived(depth, h)

        def add(there):
            psend[last, there, piece(h)] = (
                other[there, piece(h)] + chain[depth, there, piece(h)].astype(f32)
            ).astype(bf16)

        by_rows(add, rows)
        start(False, functools.partial(y_copy, last, h))

    ends = {True: (2, depth), False: (depth - 1,)}

    def lead_swap():
        return remote(lead_out, lead_in, ly_s.at[0], ly_r.at[0], flip_y)


    def cross_lead(inside):
        value = lead_own[last, pl.ds(away, rows)]
        for slot in ends[inside]:
            lead_arrived(slot)
            value = value + lead_chain[slot, pl.ds(away, rows)].astype(f32)
        lead_out[...] = value.astype(bf16)
        start(inside, lead_swap)

    def finish_lead(inside):
        lead_swap().wait_recv()
        value = lead_own[last, pl.ds(home, rows)] + lead_in[...].astype(f32)
        for slot in ends[inside]:
            value = value + lead_chain[slot, pl.ds(home, rows)].astype(f32)
        grad_ref[:, :lead] = value * scale

    def finish(inside, h):
        y_copy(last, h).wait_recv()
        for slot in ends[inside]:
            z_arrived(slot, h)

        def add(there):
            value = own[last, there, piece(h)] + ry[last, there, piece(h)].astype(f32)
            for slot in ends[inside]:
                value = value + chain[slot, there, piece(h)].astype(f32)
            grad_ref[there, piece(h)] = value * scale

        by_rows(add, rows)

    def take(inside, step):
        kind, spot = step[0], step[1:]
        if step == "own":
            spread(inside, (z, y, x, core), ROUTES[inside]["o0"])
        elif kind in "ax":
            zs, ys = places[inside][spot[0]], y if spot[1] == "0" else over_y
            if kind == "a":
                where = (zs, ys, x, core)
                arrived(where)
                spread(inside, where, ROUTES[inside].get(spot, LONE[inside]))
            else:
                where = (zs, ys, over_x, core)
                arrived(where)
                spread(inside, where, "s")
        elif kind == "L":
            lead_step(inside, int(spot))
        elif kind == "S":
            chain_step(inside, int(spot[0]), int(spot[1]))
        elif kind == "E":
            start(inside, functools.partial(extra_copy, int(spot)))
        elif kind == "y":
            start(inside, functools.partial(y_copy, int(spot[0]), int(spot[1])))
        elif step == "CL":
            cross_lead(inside)
        elif kind == "C":
            cross_step(int(spot))
        elif step == "FL":
            finish_lead(inside)
        elif kind == "F":
            finish(inside, int(spot))

    runs, joint = {True: [[]], False: [[]]}, {True: [], False: []}
    for inside, steps in ((True, INNER_STEPS), (False, OUTER_STEPS)):
        for step in steps:
            if step[0] in "BPRWM":
                joint[inside].append(step)
                runs[inside].append([])
            else:
                runs[inside][-1].append(step)

    for k in range(len(joint[True]) + 1):
        for inside in (True, False):
            if runs[inside][k]:
                @pl.when(inner if inside else jnp.logical_not(inner))
                def _():
                    for step in runs[inside][k]:
                        take(inside, step)

        if k == len(joint[True]):
            continue
        step = joint[True][k]
        if step[0] == "B":
            multiply(int(step[1]), pieces if step[2] == "L" else int(step[2]))
            if step == "B00":
                pl.semaphore_wait(barrier, 4 + jnp.where(inner, 1, 0))
        elif step[0] == "P":
            send_parts()
        elif step[0] == "R":
            relay_parts()
        elif step[0] == "W":
            outer()
        else:
            zs = jnp.where(inner, *(places[inside][joint[inside][k][1]] for inside in (True, False)))
            for ys in range(2):
                for xs in range(2):
                    arrived((zs, ys, xs, 1 - core))
            if k == len(joint[True]) - 1:
                row_ref[...] = weights[f]
            there = pl.ds(pl.multiple_of(zs * pair, 128), pair)
            block = weights[pl.ds(2 * zs, 2)].reshape(pair, width)
            back[:, there] = lax.dot_general(
                cot[...], block, (((1,), (1,)), ((), ())), preferred_element_type=f32
            ).astype(bf16)

    for k in range(3):
        part_copy(k).wait_send()
    for inside in (True, False):
        @pl.when(inner if inside else jnp.logical_not(inner))
        def _():
            for make in sends[inside]:
                make().wait_send()


def finish_kernel(
    groups, lines,
    anchor, momentum, summed, row, first, second, gradient, back,
    anchor_hbm, momentum_hbm, local_hbm, first_hbm, second_hbm, back_hbm,
    anchor_out, momentum_out, local_out, first_out, second_out, sems,
):
    copies = []

    def put(src, dst):
        copies.append(pltpu.make_async_copy(src, dst, sems.at[len(copies)]))
        copies[-1].start()

    put(back, back_hbm)
    for k in range(row.shape[0] // lines):
        there = pl.ds(k * lines, lines)
        local, first_next, second_next = adam(
            row[there].astype(f32), first[there], second[there], gradient[there]
        )
        first_out[there] = first_next
        put(first_out.at[there], first_hbm.at[there])
        second_out[there] = second_next
        put(second_out.at[there], second_hbm.at[there])
        local_out[there] = local
        put(local_out.at[there], local_hbm.at[there])
    new_anchor, new_momentum = outer_step(anchor[...], momentum[...], summed[...], groups)
    anchor_out[...] = new_anchor
    put(anchor_out, anchor_hbm)
    momentum_out[...] = new_momentum
    put(momentum_out, momentum_hbm)
    for copy in copies:
        copy.wait()


def plan(width):
    lead = width // 6 // 128 * 128
    part = width // 2 // 128 * 128
    return lead, ((lead, part), (lead + part, width - lead - part)), 1


def fused_shards(anchor, momentum, change, adam_first, adam_second, attn_out, grad_out):
    groups, devices = lax.axis_size("replica"), lax.axis_size("fsdp")
    depth = devices // 2
    rows, width = change.shape[1:]
    tokens = attn_out.shape[1]
    cols = width // groups
    lead, cuts, extras = plan(width)
    rest = width - lead
    pieces = len(cuts)
    scale = (tokens * devices) ** (-0.5)
    dma = pltpu.SemaphoreType.DMA
    vmem = pltpu.VMEM
    in_hbm = pl.BlockSpec(memory_space=pltpu.HBM)
    in_vmem = pl.BlockSpec(memory_space=pltpu.VMEM)
    summed, anchor_row, gradient, input_grad = pl.pallas_call(
        functools.partial(kernel, depth, groups, scale, lead, cuts, extras),
        out_shape=(
            jax.ShapeDtypeStruct((rows, cols), f32),
            jax.ShapeDtypeStruct((rows, width), bf16),
            jax.ShapeDtypeStruct((rows, width), f32),
            jax.ShapeDtypeStruct((tokens, width), bf16),
        ),
        in_specs=[in_hbm] * 5,
        out_specs=(in_vmem,) * 4,
        scratch_shapes=[
            vmem((rows, cols), f32),
            vmem((rows, cols), f32),
            vmem((rows, width), f32),
            vmem((depth, tokens, 2 * rows), bf16),
            vmem((tokens, width), bf16),
            vmem((2 * rows, tokens), bf16),
            vmem((3, rows, cols), bf16),
            vmem((3, rows, cols), bf16),
            vmem((depth, rows, width), f32),
            vmem((rows, width), f32),
            vmem((depth, rows, width), bf16),
            vmem((depth, rows, width), bf16),
            vmem((depth - 1, rows, width), bf16),
            vmem((depth + 1, rows, width), bf16),
            vmem((devices, rows, width), bf16),
            vmem((depth, 2 * rows, lead), f32),
            vmem((depth - 1, 2 * rows, lead), bf16),
            vmem((depth + 1, 2 * rows, lead), bf16),
            vmem((rows, lead), bf16),
            vmem((rows, lead), bf16),
            dma((depth + pieces + 4,)),
            dma((3,)), dma((3,)),
            dma((depth * pieces,)), dma((depth * pieces,)),
            dma((depth * pieces,)), dma(((depth + 1) * pieces,)),
            dma((depth - 1,)), dma((depth + 1,)), dma((1,)), dma((1,)),
            dma((5 * devices,)), dma((groups * devices,)),
        ],
        compiler_params=pltpu.CompilerParams(
            collective_id=0, has_side_effects=True, vmem_limit_bytes=38 * 2**20
        ),
    )(*(
        pltpu.with_memory_space_constraint(array, pltpu.HBM)
        for array in (anchor, momentum, change[0], attn_out[0], grad_out[0])
    ))
    lines = rows // 4
    block = jax.ShapeDtypeStruct((rows, width), f32)
    quarter = jax.ShapeDtypeStruct((rows, cols), f32)
    outs = pl.pallas_call(
        functools.partial(finish_kernel, groups, lines),
        out_shape=(
            quarter, quarter, block, block, block, jax.ShapeDtypeStruct((tokens, width), bf16),
        ),
        in_specs=[in_vmem] * 8,
        out_specs=(in_hbm,) * 6,
        scratch_shapes=[
            vmem((rows, cols), f32), vmem((rows, cols), f32),
            vmem((rows, width), f32), vmem((rows, width), f32), vmem((rows, width), f32),
            dma((3 * (rows // lines) + 3,)),
        ],
        compiler_params=pltpu.CompilerParams(vmem_limit_bytes=12 * 2**20),
    )(anchor, momentum, summed, anchor_row, adam_first[0], adam_second[0], gradient, input_grad)
    return (*outs[:2], *(out[None] for out in outs[2:]))


def shards(*arrays):
    groups, devices = lax.axis_size("replica"), lax.axis_size("fsdp")
    rows, width = arrays[2].shape[1:]
    fits = (
        groups == 4 and devices == 8 and rows % 32 == 0
        and (2 * rows) % 128 == 0 and width % (128 * groups) == 0
        and plan(width)[0] > 0
        and arrays[5].shape[1] * width <= 2**21
    )
    return (fused_shards if fits else plain_shards)(*arrays)


def solution(mesh):
    in_specs = (P("fsdp", "replica"),) * 2 + (P("replica", "fsdp", None),) * 5
    out_specs = (P("fsdp", "replica"),) * 2 + (P("replica", "fsdp", None),) * 4
    return jax.shard_map(shards, mesh=mesh, in_specs=in_specs, out_specs=out_specs, check_vma=False)
```
